32 devices in a mesh: band: 4 (over y, x), ga: 8 (over z, core).
Axes of the slice: x: 2, y: 2, z: 4, core: 2. Of those that a mesh axis runs over, the one named last changes fastest.
Arguments:
- wavefunctions: bfloat16 [512, 98304], P('band', 'ga'), may hold values from -6 to 6
- projectors: bfloat16 [2048, 98304], P('band', 'ga'), may hold values from -0.125 to 0.125
- kinetic_diag: float32 [98304], P('ga'), may hold values from 0.1 to 4
- species_index: int32 [256], replicated, may hold values from 0 to 3
- coupling: float32 [4, 8, 8], replicated, may hold values from -5 to 5
Outputs:
- applied: bfloat16 [512, 98304], P('band', 'ga')
The draws below stay inside these ranges and needn't reach their ends.
All inputs are finite; a program needn't handle non-finite values.
Results may differ from the reference program's by a relative error of at most 0.015.
Values may be sent and summed in bfloat16 or wider, within the bound.
No kernel may reach another device: no remote copies, remote signals or barrier semaphores. Data moves between devices by JAX's collectives and lax.ppermute only.
A program may use at most 64 MiB of HBM per device.

```python
import math
import jax
import jax.numpy as jnp
from jax import lax

NG = 98304
NPA = 8
ATOMS = 256
NSPEC = 4
BANDS = 512
NPROJ = 2048


def place_ends(array, rng, low, top_value):
    longest = array.shape.index(max(array.shape))
    spots = []
    for shift in (0, 1):
        where = [jax.random.randint(jax.random.fold_in(rng, axis), (), 0, length) for axis, length in enumerate(array.shape)]
        where[longest] = (where[longest] + shift) % array.shape[longest]
        spots.append(tuple(where))
    return array.at[spots[0]].set(low).at[spots[1]].set(top_value)


def shard_levels(rng, extent, split, smallest, largest):
    def one(axis_at, shards_of):
        steps = jax.random.uniform(jax.random.fold_in(jax.random.fold_in(rng, 6), axis_at), (shards_of,), jnp.float32, smallest / len(split), largest / len(split))
        return jnp.repeat(jnp.exp(steps), extent[axis_at] // shards_of).reshape((-1,) + (1,) * (len(extent) - axis_at - 1))

    gain = one(*split[0])
    for cut in split[1:]:
        gain = gain * one(*cut)
    return gain


def noise(rng, dims, spread, reach, shards=(), held_as=jnp.bfloat16):
    values = spread * jax.random.normal(rng, dims, jnp.float32)
    if shards:
        values = values * shard_levels(rng, dims, shards, -0.22, 0.18)
    return jnp.clip(values, -reach, reach).astype(held_as)


def setup_inputs(seed: int = 0) -> dict:
    splits = jax.random.split(jax.random.key(seed), 6)
    return {
        "wavefunctions": noise(splits[0], (BANDS, NG), 1.0, 6.0, ((0, 4), (1, 8))),
        "projectors": noise(splits[1], (NPROJ, NG), ((NG * NPROJ) ** -0.25), 0.125, ((0, 4), (1, 8))),
        "kinetic_diag": jnp.clip(jnp.exp(math.log(4.0) - 3.6888794 * jax.random.uniform(splits[2], (NG,), jnp.float32) ** shard_levels(splits[2], (NG,), ((0, 8),), -0.2, 0.2)), 0.1, 4.0),
        "species_index": place_ends(jax.random.randint(splits[3], (ATOMS,), 0, NSPEC), jax.random.fold_in(splits[3], 1), 0, NSPEC - 1).astype(jnp.int32),
        "coupling": noise(splits[4], (NSPEC, NPA, NPA), 0.35, 5.0, (), jnp.float32),
    }


def reference(wavefunctions, projectors, kinetic_diag, species_index, coupling):
    correlations = jnp.dot(wavefunctions, projectors.T, preferred_element_type=jnp.float32)
    onehot = (species_index[:, None] == jnp.arange(NSPEC, dtype=jnp.int32)[None, :]).astype(jnp.float32)
    blocks = jnp.einsum("as,sij->aij", onehot, coupling, precision=lax.Precision.HIGHEST)
    mixed = jnp.einsum("baj,aij->bai", correlations.reshape(BANDS, ATOMS, NPA), blocks, precision=lax.Precision.HIGHEST)
    mixed = mixed.reshape(BANDS, NPROJ).astype(jnp.bfloat16)
    nonlocal_term = jnp.dot(mixed, projectors, preferred_element_type=jnp.float32)
    return (kinetic_diag[None, :] * wavefunctions.astype(jnp.float32) + nonlocal_term).astype(jnp.bfloat16)
```

```python
import jax
import jax.numpy as jnp
from jax import lax
from jax.sharding import PartitionSpec as P

NPA = 8


def apply_blocks(correlations, species_index, coupling, atom_start):
    rows = correlations.shape[0]
    count = correlations.shape[1] // NPA
    local_species = lax.dynamic_slice_in_dim(species_index, atom_start, count)
    onehot = (
        local_species[:, None] == jnp.arange(coupling.shape[0], dtype=jnp.int32)[None, :]
    ).astype(jnp.float32)
    blocks = jnp.einsum("as,sij->aij", onehot, coupling, precision=lax.Precision.HIGHEST)
    mixed = jnp.einsum(
        "baj,aij->bai",
        correlations.reshape(rows, count, NPA),
        blocks,
        precision=lax.Precision.HIGHEST,
    )
    return mixed.reshape(rows, count * NPA).astype(jnp.bfloat16)


def local_any(wavefunctions, projectors, kinetic_diag, species_index, coupling):
    proj_local = projectors.shape[0]
    partial_value = jnp.einsum(
        "bg,pg->bp",
        lax.all_gather(wavefunctions, "band", axis=0, tiled=True),
        projectors,
        preferred_element_type=jnp.float32,
    )
    total = lax.psum(partial_value.astype(jnp.bfloat16), "ga").astype(jnp.float32)
    first_atom = lax.axis_index("band") * proj_local // NPA
    mixed = apply_blocks(total, species_index, coupling, first_atom)
    nonlocal_term = lax.psum_scatter(
        jnp.dot(mixed, projectors, preferred_element_type=jnp.float32).astype(jnp.bfloat16),
        "band",
        scatter_dimension=0,
        tiled=True,
    ).astype(jnp.float32)
    return (kinetic_diag[None, :] * wavefunctions.astype(jnp.float32) + nonlocal_term).astype(
        jnp.bfloat16
    )


def tie(value, *after):
    return lax.optimization_barrier((value, *after))[0]


def swap(parts, bit, flag):
    return [jnp.where(flag, parts[i ^ bit], part) for i, part in enumerate(parts)]


def mixing_matrix(species_index, coupling, first_atom, count):
    species = lax.dynamic_slice_in_dim(species_index, first_atom, count)
    onehot = (
        species[:, None] == jnp.arange(coupling.shape[0], dtype=jnp.int32)[None, :]
    ).astype(jnp.float32)
    blocks = jnp.einsum("as,sij->aji", onehot, coupling, precision=lax.Precision.HIGHEST)
    tall = blocks.reshape(count * NPA, NPA)
    wide = jnp.tile(tall, (1, count))
    size = count * NPA
    row = lax.broadcasted_iota(jnp.int32, (size, size), 0) // NPA
    col = lax.broadcasted_iota(jnp.int32, (size, size), 1) // NPA
    return jnp.where(row == col, wide, 0.0)


def chunk_rows(rows, ga):
    step = max(rows // 4, ga * 4)
    return [(first, step) for first in range(0, rows, step)]


def local_square(nga, W, Pr, kinetic, species_index, coupling):
    bf, f32 = jnp.bfloat16, jnp.float32
    rows, width = W.shape
    quarter = width // 4
    block = Pr.shape[0]
    nz = nga // 2

    band = lax.axis_index("band")
    ga = lax.axis_index("ga")
    x, y = band % 2, band // 2
    core, z = ga % 2, ga // 2
    onx, ony = x == 1, y == 1

    def band_swap(value, bit):
        return lax.ppermute(value, "band", [(i, i ^ bit) for i in range(4)])

    def ga_swap(value, bit):
        return lax.ppermute(value, "ga", [(i, i ^ bit) for i in range(nga)])

    def cut(value, which):
        return lax.dynamic_slice_in_dim(value, which * quarter, quarter, axis=1)

    keep_x, give_x, keep_y, give_y = x, 1 - x, 2 + y, 3 - y

    def dot_cc(a, b):
        return lax.dot_general(a, b, (((1,), (1,)), ((), ())), preferred_element_type=f32)

    def dot_cr(a, b):
        return lax.dot_general(a, b, (((1,), (0,)), ((), ())), preferred_element_type=f32)

    chunks = chunk_rows(rows, nga)

    def send_direct(first, count, *after):
        part = lax.slice_in_dim(W, first, first + count, axis=0)
        own_x, own_y = cut(part, keep_x), cut(part, keep_y)
        out_x = jnp.concatenate([cut(part, give_x), own_y], axis=1)
        out_y = jnp.concatenate([cut(part, give_y), own_x], axis=1)
        if after:
            out_x, out_y = tie(out_x, *after), tie(out_y, *after)
        return own_x, own_y, band_swap(out_x, 1), band_swap(out_y, 2)

    def send_forward(own_x, own_y, from_x, from_y):
        near_x, near_y = from_x[:, :quarter], from_y[:, :quarter]
        far_y = band_swap(near_x, 2)
        far_x = band_swap(near_y, 1)
        wx = [own_x, near_x, from_y[:, quarter:], far_y]
        wy = [own_y, from_x[:, quarter:], near_y, far_x]
        return wx, wy

    def absolute(parts):
        return jnp.concatenate(swap(swap(parts, 1, onx), 2, ony), axis=0)

    direct = [send_direct(*chunks[0])]
    px_keep, py_keep = cut(Pr, keep_x), cut(Pr, keep_y)
    px_give = tie(cut(Pr, give_x), direct[0][0])
    py_give = tie(cut(Pr, give_y), direct[0][1])
    px_near = band_swap(px_give, 1)
    py_near = band_swap(py_give, 2)

    first_atom = band * block // NPA
    matrix = mixing_matrix(species_index, coupling, first_atom, block // NPA)

    gathered = []
    for i, (first, count) in enumerate(chunks):
        gathered.append(send_forward(*direct[i]))
        if i + 1 < len(chunks):
            after = () if i == 0 else (gathered[i - 1][0][3], gathered[i - 1][1][3])
            direct.append(send_direct(*chunks[i + 1], *after))

    outs = []
    for i, (first, count) in enumerate(chunks):
        wx, wy = absolute(gathered[i][0]), absolute(gathered[i][1])
        c_own = dot_cc(wx, px_keep) + dot_cc(wy, py_keep)
        c_x, c_y = dot_cc(wx, px_near), dot_cc(wy, py_near)
        part = jnp.concatenate([c_own.astype(bf), c_x.astype(bf), c_y.astype(bf)], axis=1)

        piece = 4 * count // nga
        part = part.reshape(nz, 2, piece, 3 * block)
        kept = lax.dynamic_index_in_dim(part, core, 1, keepdims=False)
        sent = lax.dynamic_index_in_dim(part, 1 - core, 1, keepdims=False)
        half = (kept.astype(f32) + ga_swap(sent, 1).astype(f32)).astype(bf)
        total = lax.dynamic_index_in_dim(half, z, 0, keepdims=False).astype(f32)
        for m in range(1, nz):
            out = lax.dynamic_index_in_dim(half, z ^ m, 0, keepdims=False)
            total = total + ga_swap(out, 2 * m).astype(f32)

        to_x = total[:, block : 2 * block].astype(bf)
        to_y = total[:, 2 * block :].astype(bf)
        correlations = (
            total[:, :block] + band_swap(to_x, 1).astype(f32) + band_swap(to_y, 2).astype(f32)
        )
        mixed = jnp.dot(correlations, matrix, precision=lax.Precision.HIGHEST).astype(bf)
        mixed = jnp.concatenate([mixed, band_swap(mixed, 1), band_swap(mixed, 2)], axis=1)

        parts = [mixed] + [ga_swap(mixed, 2 * m) for m in range(1, nz)]
        bit = 1
        while bit < nz:
            parts = swap(parts, bit, (z & bit) != 0)
            bit *= 2
        mine = jnp.stack(parts)
        other = ga_swap(mine, 1)
        both = swap([mine, other], 1, core == 1)
        every = jnp.stack(both, axis=1).reshape(4, count, 3 * block)
        every = jnp.concatenate(swap(swap(list(every), 1, onx), 2, ony), axis=0)

        m_own, m_x, m_y = (every[:, k * block : (k + 1) * block] for k in range(3))
        ox = dot_cr(m_own, px_keep) + dot_cr(m_x, px_near)
        oy = dot_cr(m_own, py_keep) + dot_cr(m_y, py_near)

        def own(value, k):
            return value[k * count : (k + 1) * count]

        ox_next = own(ox, 1) + band_swap(own(ox, 3).astype(bf), 2).astype(f32)
        oy_next = own(oy, 2) + band_swap(own(oy, 3).astype(bf), 1).astype(f32)
        ox_here = own(ox, 0) + band_swap(own(ox, 2).astype(bf), 2).astype(f32)
        oy_here = own(oy, 0) + band_swap(own(oy, 1).astype(bf), 1).astype(f32)
        ox_far = band_swap(ox_next.astype(bf), 1).astype(f32)
        oy_far = band_swap(oy_next.astype(bf), 2).astype(f32)

        terms = swap([ox_here, ox_far], 1, onx) + swap([oy_here, oy_far], 1, ony)
        part = lax.slice_in_dim(W, first, first + count, axis=0).astype(f32)
        outs.append(
            (kinetic[None, :] * part + jnp.concatenate(terms, axis=1)).astype(bf)
        )
    return jnp.concatenate(outs, axis=0)


def solution(mesh):
    in_specs = (P("band", "ga"), P("band", "ga"), P("ga"), P(), P())
    out_specs = P("band", "ga")
    nband, nga = mesh.shape["band"], mesh.shape["ga"]

    def local(*args):
        if nband == 4 and nga % 2 == 0 and nga & (nga - 1) == 0:
            return local_square(nga, *args)
        return local_any(*args)

    return jax.shard_map(local, mesh=mesh, in_specs=in_specs, out_specs=out_specs, check_vma=False)
```

```python
import functools

import jax
import jax.numpy as jnp
from jax import lax
from jax.experimental import pallas as pl
from jax.experimental.pallas import tpu as pltpu
from jax.sharding import PartitionSpec as P


NPA = 8


def apply_blocks(correlations, species_index, coupling, atom_start):
    rows = correlations.shape[0]
    count = correlations.shape[1] // NPA
    local_species = lax.dynamic_slice_in_dim(species_index, atom_start, count)
    onehot = (
        local_species[:, None] == jnp.arange(coupling.shape[0], dtype=jnp.int32)[None, :]
    ).astype(jnp.float32)
    blocks = jnp.einsum("as,sij->aij", onehot, coupling, precision=lax.Precision.HIGHEST)
    mixed = jnp.einsum(
        "baj,aij->bai",
        correlations.reshape(rows, count, NPA),
        blocks,
        precision=lax.Precision.HIGHEST,
    )
    return mixed.reshape(rows, count * NPA).astype(jnp.bfloat16)


def local_any(wavefunctions, projectors, kinetic_diag, species_index, coupling):
    proj_local = projectors.shape[0]
    partial_value = jnp.einsum(
        "bg,pg->bp",
        lax.all_gather(wavefunctions, "band", axis=0, tiled=True),
        projectors,
        preferred_element_type=jnp.float32,
    )
    total = lax.psum(partial_value.astype(jnp.bfloat16), "ga").astype(jnp.float32)
    first_atom = lax.axis_index("band") * proj_local // NPA
    mixed = apply_blocks(total, species_index, coupling, first_atom)
    nonlocal_term = lax.psum_scatter(
        jnp.dot(mixed, projectors, preferred_element_type=jnp.float32).astype(jnp.bfloat16),
        "band",
        scatter_dimension=0,
        tiled=True,
    ).astype(jnp.float32)
    return (kinetic_diag[None, :] * wavefunctions.astype(jnp.float32) + nonlocal_term).astype(
        jnp.bfloat16
    )


def swap(parts, bit, flag):
    return [jnp.where(flag, parts[i ^ bit], part) for i, part in enumerate(parts)]


def mixing_matrix(species_index, coupling, first_atom, count):
    species = lax.dynamic_slice_in_dim(species_index, first_atom, count)
    onehot = (
        species[:, None] == jnp.arange(coupling.shape[0], dtype=jnp.int32)[None, :]
    ).astype(jnp.float32)
    blocks = jnp.einsum("as,sij->aji", onehot, coupling, precision=lax.Precision.HIGHEST)
    tall = blocks.reshape(count * NPA, NPA)
    wide = jnp.tile(tall, (1, count))
    size = count * NPA
    row = lax.broadcasted_iota(jnp.int32, (size, size), 0) // NPA
    col = lax.broadcasted_iota(jnp.int32, (size, size), 1) // NPA
    return jnp.where(row == col, wide, 0.0)


def chunk_rows(rows, ga):
    unit = max(32, ga * 4)
    if rows % (4 * unit):
        return [(0, rows)]
    return [(0, rows // 4), (rows // 4, rows // 2), (3 * rows // 4, rows // 4)]


def stage_order(n):
    order = [("Wd", 0), ("We", 0), ("T", 0), ("Wf", 0), ("Wd", 1), ("We", 1), ("A", 0), ("B", 0)]
    order += [("Wf", 1), ("Wd", 2), ("We", 2)]
    for c in range(n):
        order += [("A", c), ("Wf", c + 1), ("B", c), ("C", c)]
        order += [("I", c - 2), ("H", c - 1), ("E", c), ("G", c), ("K", c), ("Wd", c + 3), ("We", c + 3)]
    order += [("I", n - 2), ("H", n - 1), ("I", n - 1)]
    seen, kept = set(), []
    for item in order:
        if 0 <= item[1] < n and item not in seen:
            seen.add(item)
            kept.append(item)
    return kept


def tile_of(width, parts=4):
    while parts > 1 and width % (128 * parts):
        parts -= 1
    return width // parts


def piece_row(piece, rows, index, band):
    first = index * piece
    return pl.multiple_of(((first // rows) ^ band) * rows + first % rows, piece)


def transpose_kernel(value, out):
    out[...] = value[...].T


def transpose(value):
    block, width = value.shape
    tile = tile_of(width, 12)
    return pl.pallas_call(
        transpose_kernel,
        grid=(width // tile,),
        in_specs=[pl.BlockSpec((block, tile), lambda k: (0, k))],
        out_specs=pl.BlockSpec((tile, block), lambda k: (k, 0)),
        out_shape=jax.ShapeDtypeStruct((width, block), value.dtype),
        cost_estimate=pl.CostEstimate(
            flops=16 * block * width, bytes_accessed=4 * block * width, transcendentals=0
        ),
        name="transpose",
    )(value)


def correlate_kernel(nz, where, *refs):
    halves, (proj, kept, sent, acc) = refs[:8], refs[8:]
    step = pl.program_id(0)
    band, core = where[0], where[1]
    bands = jnp.concatenate([half[...] for half in halves], axis=0)
    part = jnp.dot(bands, proj[...], preferred_element_type=jnp.float32)

    @pl.when(step == 0)
    def _():
        acc[...] = part

    @pl.when(step > 0)
    def _():
        acc[...] += part

    @pl.when(step == pl.num_programs(0) - 1)
    def _():
        rows = 2 * halves[0].shape[0]
        piece = kept.shape[1]
        for k in range(nz):
            at = piece_row(piece, rows, 2 * k + core, band)
            kept[k] = acc[pl.ds(at, piece), :].astype(kept.dtype)
            at = piece_row(piece, rows, 2 * k + 1 - core, band)
            sent[k] = acc[pl.ds(at, piece), :].astype(sent.dtype)


def correlate(where, nz, halves, proj):
    half, width = halves[0].shape
    block = proj.shape[1]
    piece = 8 * half // (2 * nz)
    tile = tile_of(width)
    out = jax.ShapeDtypeStruct((nz, piece, block), jnp.bfloat16)
    whole = pl.BlockSpec((nz, piece, block), lambda k, w: (0, 0, 0))
    return pl.pallas_call(
        functools.partial(correlate_kernel, nz),
        grid_spec=pltpu.PrefetchScalarGridSpec(
            num_scalar_prefetch=1,
            grid=(width // tile,),
            in_specs=[pl.BlockSpec((half, tile), lambda k, w: (0, k))] * 8
            + [pl.BlockSpec((tile, block), lambda k, w: (k, 0))],
            out_specs=[whole, whole],
            scratch_shapes=[pltpu.VMEM((8 * half, block), jnp.float32)],
        ),
        out_shape=[out, out],
        cost_estimate=pl.CostEstimate(
            flops=16 * half * width * block,
            bytes_accessed=2 * (8 * half + block) * width,
            transcendentals=0,
        ),
        name="correlate",
    )(where, *halves, proj)


def expand_kernel(nz, where, here, there, proj, *refs):
    outs, (pieces, mixed) = refs[:8], refs[8:]
    band, core = where[0], where[1]
    half = outs[0].shape[0]
    rows = 2 * half
    piece = here.shape[1]

    @pl.when(pl.program_id(0) == 0)
    def _():
        for k in range(nz):
            pieces[piece_row(piece, rows, 2 * k + core, band) // piece] = here[k]
            pieces[piece_row(piece, rows, 2 * k + 1 - core, band) // piece] = there[k]
        mixed[...] = jnp.concatenate([pieces[k] for k in range(2 * nz)], axis=0)

    value = jnp.dot(mixed[...], proj[...], preferred_element_type=jnp.float32)
    for k, out in enumerate(outs):
        out[...] = value[k * half : (k + 1) * half].astype(out.dtype)


def expand(where, nz, rows, here, there, proj):
    block, width = proj.shape
    piece = here.shape[1]
    tile = tile_of(width)
    whole = pl.BlockSpec((nz, piece, block), lambda k, w: (0, 0, 0))

    def out(count):
        return jax.ShapeDtypeStruct((count, width), jnp.bfloat16)

    def spec(count):
        return pl.BlockSpec((count, tile), lambda k, w: (0, k))

    counts = [rows // 2] * 8
    return pl.pallas_call(
        functools.partial(expand_kernel, nz),
        grid_spec=pltpu.PrefetchScalarGridSpec(
            num_scalar_prefetch=1,
            grid=(width // tile,),
            in_specs=[whole, whole, spec(block)],
            out_specs=[spec(n) for n in counts],
            scratch_shapes=[
                pltpu.VMEM((2 * nz, piece, block), jnp.bfloat16),
                pltpu.VMEM((4 * rows, block), jnp.bfloat16),
            ],
        ),
        out_shape=[out(n) for n in counts],
        cost_estimate=pl.CostEstimate(
            flops=8 * rows * width * block,
            bytes_accessed=2 * (4 * rows + block) * width,
            transcendentals=0,
        ),
        name="expand",
    )(where, here, there, proj)


def local_square(nga, W, Pr, kinetic, species_index, coupling):
    bf, f32 = jnp.bfloat16, jnp.float32
    rows, _ = W.shape
    block = Pr.shape[0]
    nz = nga // 2

    band = lax.axis_index("band")
    ga = lax.axis_index("ga")
    core, z = ga % 2, ga // 2
    where = jnp.stack([band, core])

    def band_swap(value, bit):
        return lax.ppermute(value, "band", [(i, i ^ bit) for i in range(4)])

    def ga_swap(value, bit):
        return lax.ppermute(value, "ga", [(i, i ^ bit) for i in range(nga)])

    chunks = chunk_rows(rows, nga)
    matrix = mixing_matrix(species_index, coupling, band * block // NPA, block // NPA)
    clock = [()]

    def now(*values):
        out = lax.optimization_barrier((*values, *clock[0]))
        return out[: len(values)]

    state = [dict() for _ in chunks]
    shared = {"out": jnp.zeros_like(W)}

    def stage_Wd(c, s):
        first, count = chunks[c]
        half = count // 2
        (bands,) = now(W)
        s["own"] = [lax.slice_in_dim(bands, at, at + half, axis=0) for at in (first, first + half)]
        s["x0"] = band_swap(s["own"][0], 1)
        s["y1"] = band_swap(s["own"][1], 2)
        return tuple(s["own"])

    def stage_We(c, s):
        own = now(*s["own"])
        s["x1"] = band_swap(own[1], 1)
        s["y0"] = band_swap(own[0], 2)
        return tuple(own)

    def stage_T(c, s):
        (turned,) = now(Pr)
        shared["turned"] = transpose(turned)
        return (shared["turned"],)

    def stage_Wf(c, s):
        x0, y1 = now(s["x0"], s["y1"])
        s["far0"] = band_swap(x0, 2)
        s["far1"] = band_swap(y1, 1)
        return x0, y1

    def stage_A(c, s):
        x1, y0, far0, far1 = now(s["x1"], s["y0"], s["far0"], s["far1"])
        halves = [*s["own"], s["x0"], x1, y0, s["y1"], far0, far1]
        s["kept"], sent = correlate(where, nz, halves, shared["turned"])
        s["core"] = ga_swap(sent, 1)
        return s["kept"], sent

    def stage_B(c, s):
        (other,) = now(s["core"])
        half = (s["kept"].astype(f32) + other.astype(f32)).astype(bf)
        outs = [
            lax.dynamic_index_in_dim(half, z ^ m, 0, keepdims=False) for m in range(1, nz)
        ]
        s["mine"] = lax.dynamic_index_in_dim(half, z, 0, keepdims=False)
        s["z"] = [ga_swap(out, 2 * m) for m, out in enumerate(outs, 1)]
        return tuple(outs)

    def stage_C(c, s):
        parts = now(*s["z"])
        total = s["mine"].astype(f32)
        for part in parts:
            total = total + part.astype(f32)
        mixed = jnp.dot(total, matrix, precision=lax.Precision.HIGHEST).astype(bf)
        s["mixed"] = [mixed] + [ga_swap(mixed, 2 * m) for m in range(1, nz)]
        return (mixed,)

    def stage_E(c, s):
        parts = list(now(*s["mixed"]))
        bit = 1
        while bit < nz:
            parts = swap(parts, bit, (z & bit) != 0)
            bit *= 2
        s["here"] = jnp.stack(parts)
        s["there"] = ga_swap(s["here"], 1)
        return (s["here"],)

    def stage_G(c, s):
        here, there = now(s["here"], s["there"])
        s["o"] = expand(where, nz, chunks[c][1], here, there, Pr)
        s["first_y"] = band_swap(s["o"][6], 2)
        s["first_x"] = band_swap(s["o"][7], 1)
        return s["o"][6], s["o"][7]

    def stage_K(c, s):
        to_y, to_x = now(s["o"][4], s["o"][3])
        s["near0"] = band_swap(to_y, 2)
        s["near1"] = band_swap(to_x, 1)
        return to_y, to_x

    def stage_H(c, s):
        first_x, first_y = now(s["first_x"], s["first_y"])
        to_x = (s["o"][2].astype(f32) + first_y.astype(f32)).astype(bf)
        to_y = (s["o"][5].astype(f32) + first_x.astype(f32)).astype(bf)
        s["second0"] = band_swap(to_x, 1)
        s["second1"] = band_swap(to_y, 2)
        return to_x, to_y

    def stage_I(c, s):
        parts = now(s["near0"], s["near1"], s["second0"], s["second1"])
        first, count = chunks[c]
        done = []
        for k in range(2):
            own = s["o"][k].astype(f32) + parts[k].astype(f32) + parts[2 + k].astype(f32)
            at = first + k * (count // 2)
            bands = lax.slice_in_dim(W, at, at + count // 2, axis=0).astype(f32)
            done.append((kinetic[None, :] * bands + own).astype(bf))
            shared["out"] = lax.dynamic_update_slice(shared["out"], done[k], (at, 0))
        return tuple(done)

    stages = dict(
        Wd=stage_Wd, We=stage_We, T=stage_T, Wf=stage_Wf, A=stage_A, B=stage_B, C=stage_C,
        E=stage_E, G=stage_G, K=stage_K, H=stage_H, I=stage_I,
    )
    for name, c in stage_order(len(chunks)):
        clock[0] = stages[name](c, state[c])
    return shared["out"]


def solution(mesh):
    in_specs = (P("band", "ga"), P("band", "ga"), P("ga"), P(), P())
    out_specs = P("band", "ga")
    nband, nga = mesh.shape["band"], mesh.shape["ga"]
    square = nband == 4 and nga >= 4 and nga & (nga - 1) == 0

    def local(*args):
        return local_square(nga, *args) if square else local_any(*args)

    def step(*args):
        f = jax.shard_map(
            local, mesh=mesh, in_specs=in_specs, out_specs=out_specs, check_vma=False
        )
        return f(*args)

    return step
```

```python
import functools

import jax
import jax.numpy as jnp
from jax import lax
from jax.experimental import pallas as pl
from jax.experimental.pallas import tpu as pltpu
from jax.sharding import PartitionSpec as P


NPA = 8


def apply_blocks(correlations, species_index, coupling, atom_start):
    rows = correlations.shape[0]
    count = correlations.shape[1] // NPA
    local_species = lax.dynamic_slice_in_dim(species_index, atom_start, count)
    onehot = (
        local_species[:, None] == jnp.arange(coupling.shape[0], dtype=jnp.int32)[None, :]
    ).astype(jnp.float32)
    blocks = jnp.einsum("as,sij->aij", onehot, coupling, precision=lax.Precision.HIGHEST)
    mixed = jnp.einsum(
        "baj,aij->bai",
        correlations.reshape(rows, count, NPA),
        blocks,
        precision=lax.Precision.HIGHEST,
    )
    return mixed.reshape(rows, count * NPA).astype(jnp.bfloat16)


def local_any(wavefunctions, projectors, kinetic_diag, species_index, coupling):
    proj_local = projectors.shape[0]
    partial_value = jnp.einsum(
        "bg,pg->bp",
        lax.all_gather(wavefunctions, "band", axis=0, tiled=True),
        projectors,
        preferred_element_type=jnp.float32,
    )
    total = lax.psum(partial_value.astype(jnp.bfloat16), "ga").astype(jnp.float32)
    first_atom = lax.axis_index("band") * proj_local // NPA
    mixed = apply_blocks(total, species_index, coupling, first_atom)
    nonlocal_term = lax.psum_scatter(
        jnp.dot(mixed, projectors, preferred_element_type=jnp.float32).astype(jnp.bfloat16),
        "band",
        scatter_dimension=0,
        tiled=True,
    ).astype(jnp.float32)
    return (kinetic_diag[None, :] * wavefunctions.astype(jnp.float32) + nonlocal_term).astype(
        jnp.bfloat16
    )


def swap(parts, bit, flag):
    return [jnp.where(flag, parts[i ^ bit], part) for i, part in enumerate(parts)]


def mixing_matrix(species_index, coupling, first_atom, count):
    species = lax.dynamic_slice_in_dim(species_index, first_atom, count)
    onehot = (
        species[:, None] == jnp.arange(coupling.shape[0], dtype=jnp.int32)[None, :]
    ).astype(jnp.float32)
    blocks = jnp.einsum("as,sij->aji", onehot, coupling, precision=lax.Precision.HIGHEST)
    tall = blocks.reshape(count * NPA, NPA)
    wide = jnp.tile(tall, (1, count))
    size = count * NPA
    row = lax.broadcasted_iota(jnp.int32, (size, size), 0) // NPA
    col = lax.broadcasted_iota(jnp.int32, (size, size), 1) // NPA
    return jnp.where(row == col, wide, 0.0)


def chunk_rows(rows, ga):
    unit = max(32, ga * 4)
    if rows % (4 * unit):
        return [(0, rows)]
    return [(rows // 2, rows // 4), (0, rows // 2), (3 * rows // 4, rows // 4)]


def stage_order(n):
    order = [("Wd", 0), ("We", 0), ("T", 0), ("Wf", 0), ("Wd", 1), ("We", 1), ("M", 0)]
    order += [("A", 0), ("B", 0), ("Wf", 1), ("Wd", 2), ("We", 2)]
    for c in range(n):
        order += [("A", c), ("Wf", c + 1), ("B", c), ("C", c)]
        order += [("H", c - 1), ("E", c), ("G", c), ("K", c), ("Wd", c + 3), ("We", c + 3)]
    order += [("I", c) for c in range(n - 1)]
    order += [("H", n - 1), ("I", n - 1)]
    seen, kept = set(), []
    for item in order:
        if 0 <= item[1] < n and item not in seen:
            seen.add(item)
            kept.append(item)
    return kept


def tile_of(width, parts=4):
    while parts > 1 and width % (128 * parts):
        parts -= 1
    return width // parts


def piece_row(piece, rows, index, band):
    first = index * piece
    return pl.multiple_of(((first // rows) ^ band) * rows + first % rows, piece)


def transpose_kernel(value, out):
    out[...] = value[...].T


def transpose(value):
    block, width = value.shape
    tile = tile_of(width, 12)
    return pl.pallas_call(
        transpose_kernel,
        grid=(width // tile,),
        in_specs=[pl.BlockSpec((block, tile), lambda k: (0, k))],
        out_specs=pl.BlockSpec((tile, block), lambda k: (k, 0)),
        out_shape=jax.ShapeDtypeStruct((width, block), value.dtype),
        cost_estimate=pl.CostEstimate(
            flops=16 * block * width, bytes_accessed=4 * block * width, transcendentals=0
        ),
        name="transpose",
    )(value)


def halves_kernel(value, first, second):
    half = first.shape[0]
    first[...] = value[:half]
    second[...] = value[half:]


def take_halves(value, first, count):
    width = value.shape[1]
    tile = tile_of(width, 2)
    return pl.pallas_call(
        halves_kernel,
        grid=(width // tile,),
        in_specs=[pl.BlockSpec((count, tile), lambda k: (first // count, k))],
        out_specs=[pl.BlockSpec((count // 2, tile), lambda k: (0, k))] * 2,
        out_shape=[jax.ShapeDtypeStruct((count // 2, width), value.dtype)] * 2,
        cost_estimate=pl.CostEstimate(
            flops=count * width, bytes_accessed=4 * count * width, transcendentals=0
        ),
        name="take",
    )(value)


def join_kernel(a, b, c, d, first, second):
    f32 = jnp.float32
    first[...] = (a[...].astype(f32) + b[...].astype(f32)).astype(first.dtype)
    second[...] = (c[...].astype(f32) + d[...].astype(f32)).astype(second.dtype)


def join(a, b, c, d):
    half, width = a.shape
    tile = tile_of(width, 2)
    spec = pl.BlockSpec((half, tile), lambda k: (0, k))
    return pl.pallas_call(
        join_kernel,
        grid=(width // tile,),
        in_specs=[spec] * 4,
        out_specs=[spec] * 2,
        out_shape=[jax.ShapeDtypeStruct(a.shape, a.dtype)] * 2,
        cost_estimate=pl.CostEstimate(
            flops=2 * half * width, bytes_accessed=12 * half * width, transcendentals=0
        ),
        name="join",
    )(a, b, c, d)


def finish_kernel(bands, kinetic, *refs):
    terms, out = refs[:6], refs[-1]
    half = terms[0].shape[0]
    f32 = jnp.float32
    for k in range(2):
        rows = slice(k * half, (k + 1) * half)
        own = sum(term[...].astype(f32) for term in terms[k::2])
        out[rows] = (kinetic[...] * bands[rows].astype(f32) + own).astype(out.dtype)


def finish(bands, kinetic, terms, first, out):
    half, width = terms[0].shape
    count = 2 * half
    tile = tile_of(width, 2)
    rows = pl.BlockSpec((count, tile), lambda k: (first // count, k))
    part = pl.BlockSpec((half, tile), lambda k: (0, k))
    args = [bands, kinetic[None, :], *terms]
    specs = [rows, pl.BlockSpec((1, tile), lambda k: (0, k))] + [part] * 6
    aliases = {}
    if out is not None:
        aliases = {len(args): 0}
        args.append(out)
        specs.append(pl.BlockSpec(memory_space=pl.ANY))
    return pl.pallas_call(
        finish_kernel,
        grid=(width // tile,),
        in_specs=specs,
        out_specs=rows,
        out_shape=jax.ShapeDtypeStruct(bands.shape, bands.dtype),
        input_output_aliases=aliases,
        cost_estimate=pl.CostEstimate(
            flops=8 * count * width, bytes_accessed=10 * count * width, transcendentals=0
        ),
        name="finish",
    )(*args)


def correlate_kernel(nz, where, *refs):
    halves, (proj, kept, sent, acc) = refs[:8], refs[8:]
    step = pl.program_id(0)
    band, core = where[0], where[1]
    bands = jnp.concatenate([half[...] for half in halves], axis=0)
    part = jnp.dot(bands, proj[...], preferred_element_type=jnp.float32)

    @pl.when(step == 0)
    def _():
        acc[...] = part

    @pl.when(step > 0)
    def _():
        acc[...] += part

    @pl.when(step == pl.num_programs(0) - 1)
    def _():
        rows = 2 * halves[0].shape[0]
        piece = kept.shape[1]
        for k in range(nz):
            at = piece_row(piece, rows, 2 * k + core, band)
            kept[k] = acc[pl.ds(at, piece), :].astype(kept.dtype)
            at = piece_row(piece, rows, 2 * k + 1 - core, band)
            sent[k] = acc[pl.ds(at, piece), :].astype(sent.dtype)


def correlate(where, nz, halves, proj):
    half, width = halves[0].shape
    block = proj.shape[1]
    piece = 8 * half // (2 * nz)
    tile = tile_of(width)
    out = jax.ShapeDtypeStruct((nz, piece, block), jnp.bfloat16)
    whole = pl.BlockSpec((nz, piece, block), lambda k, w: (0, 0, 0))
    return pl.pallas_call(
        functools.partial(correlate_kernel, nz),
        grid_spec=pltpu.PrefetchScalarGridSpec(
            num_scalar_prefetch=1,
            grid=(width // tile,),
            in_specs=[pl.BlockSpec((half, tile), lambda k, w: (0, k))] * 8
            + [pl.BlockSpec((tile, block), lambda k, w: (k, 0))],
            out_specs=[whole, whole],
            scratch_shapes=[pltpu.VMEM((8 * half, block), jnp.float32)],
        ),
        out_shape=[out, out],
        cost_estimate=pl.CostEstimate(
            flops=16 * half * width * block,
            bytes_accessed=2 * (8 * half + block) * width,
            transcendentals=0,
        ),
        name="correlate",
    )(where, *halves, proj)


def expand_kernel(nz, where, here, there, proj, *refs):
    outs, (pieces, mixed) = refs[:8], refs[8:]
    band, core = where[0], where[1]
    half = outs[0].shape[0]
    rows = 2 * half
    piece = here.shape[1]

    @pl.when(pl.program_id(0) == 0)
    def _():
        for k in range(nz):
            pieces[piece_row(piece, rows, 2 * k + core, band) // piece] = here[k]
            pieces[piece_row(piece, rows, 2 * k + 1 - core, band) // piece] = there[k]
        mixed[...] = jnp.concatenate([pieces[k] for k in range(2 * nz)], axis=0)

    value = jnp.dot(mixed[...], proj[...], preferred_element_type=jnp.float32)
    for k, out in enumerate(outs):
        out[...] = value[k * half : (k + 1) * half].astype(out.dtype)


def expand(where, nz, rows, here, there, proj):
    block, width = proj.shape
    piece = here.shape[1]
    tile = tile_of(width)
    whole = pl.BlockSpec((nz, piece, block), lambda k, w: (0, 0, 0))

    def out(count):
        return jax.ShapeDtypeStruct((count, width), jnp.bfloat16)

    def spec(count):
        return pl.BlockSpec((count, tile), lambda k, w: (0, k))

    counts = [rows // 2] * 8
    return pl.pallas_call(
        functools.partial(expand_kernel, nz),
        grid_spec=pltpu.PrefetchScalarGridSpec(
            num_scalar_prefetch=1,
            grid=(width // tile,),
            in_specs=[whole, whole, spec(block)],
            out_specs=[spec(n) for n in counts],
            scratch_shapes=[
                pltpu.VMEM((2 * nz, piece, block), jnp.bfloat16),
                pltpu.VMEM((4 * rows, block), jnp.bfloat16),
            ],
        ),
        out_shape=[out(n) for n in counts],
        cost_estimate=pl.CostEstimate(
            flops=8 * rows * width * block,
            bytes_accessed=2 * (4 * rows + block) * width,
            transcendentals=0,
        ),
        name="expand",
    )(where, here, there, proj)


def local_square(nga, W, Pr, kinetic, species_index, coupling):
    bf, f32 = jnp.bfloat16, jnp.float32
    rows, _ = W.shape
    block = Pr.shape[0]
    nz = nga // 2

    band = lax.axis_index("band")
    ga = lax.axis_index("ga")
    core, z = ga % 2, ga // 2
    where = jnp.stack([band, core])

    def band_swap(value, bit):
        return lax.ppermute(value, "band", [(i, i ^ bit) for i in range(4)])

    def ga_swap(value, bit):
        return lax.ppermute(value, "ga", [(i, i ^ bit) for i in range(nga)])

    chunks = chunk_rows(rows, nga)
    clock = [()]

    def now(*values):
        out = lax.optimization_barrier((*values, *clock[0]))
        return out[: len(values)]

    state = [dict() for _ in chunks]
    shared = {}

    def stage_Wd(c, s):
        first, count = chunks[c]
        (bands,) = now(W)
        s["own"] = take_halves(bands, first, count)
        s["x0"] = band_swap(s["own"][0], 1)
        s["y1"] = band_swap(s["own"][1], 2)
        return tuple(s["own"])

    def stage_We(c, s):
        own = now(*s["own"])
        s["x1"] = band_swap(own[1], 1)
        s["y0"] = band_swap(own[0], 2)
        return tuple(own)

    def stage_T(c, s):
        (turned,) = now(Pr)
        shared["turned"] = transpose(turned)
        return (shared["turned"],)

    def stage_Wf(c, s):
        x0, y1 = now(s["x0"], s["y1"])
        s["far0"] = band_swap(x0, 2)
        s["far1"] = band_swap(y1, 1)
        return x0, y1

    def stage_A(c, s):
        x1, y0, far0, far1 = now(s["x1"], s["y0"], s["far0"], s["far1"])
        halves = [*s["own"], s["x0"], x1, y0, s["y1"], far0, far1]
        s["kept"], sent = correlate(where, nz, halves, shared["turned"])
        s["core"] = ga_swap(sent, 1)
        return s["kept"], sent

    def stage_B(c, s):
        (other,) = now(s["core"])
        half = (s["kept"].astype(f32) + other.astype(f32)).astype(bf)
        outs = [
            lax.dynamic_index_in_dim(half, z ^ m, 0, keepdims=False) for m in range(1, nz)
        ]
        s["mine"] = lax.dynamic_index_in_dim(half, z, 0, keepdims=False)
        s["z"] = [ga_swap(out, 2 * m) for m, out in enumerate(outs, 1)]
        return tuple(outs)

    def stage_C(c, s):
        parts = now(*s["z"])
        total = s["mine"].astype(f32)
        for part in parts:
            total = total + part.astype(f32)
        mixed = jnp.dot(total, shared["matrix"], precision=lax.Precision.HIGHEST).astype(bf)
        s["mixed"] = [mixed] + [ga_swap(mixed, 2 * m) for m in range(1, nz)]
        return (mixed,)

    def stage_E(c, s):
        parts = list(now(*s["mixed"]))
        bit = 1
        while bit < nz:
            parts = swap(parts, bit, (z & bit) != 0)
            bit *= 2
        s["here"] = jnp.stack(parts)
        s["there"] = ga_swap(s["here"], 1)
        return (s["here"],)

    def stage_G(c, s):
        here, there = now(s["here"], s["there"])
        s["o"] = expand(where, nz, chunks[c][1], here, there, Pr)
        s["first_y"] = band_swap(s["o"][6], 2)
        s["first_x"] = band_swap(s["o"][7], 1)
        return s["o"][6], s["o"][7]

    def stage_K(c, s):
        to_y, to_x = now(s["o"][4], s["o"][3])
        s["near0"] = band_swap(to_y, 2)
        s["near1"] = band_swap(to_x, 1)
        return to_y, to_x

    def stage_H(c, s):
        first_x, first_y = now(s["first_x"], s["first_y"])
        to_x, to_y = join(s["o"][2], first_y, s["o"][5], first_x)
        s["second0"] = band_swap(to_x, 1)
        s["second1"] = band_swap(to_y, 2)
        return to_x, to_y

    def stage_I(c, s):
        parts = now(s["near0"], s["near1"], s["second0"], s["second1"])
        terms = [s["o"][0], s["o"][1], *parts]
        shared["out"] = finish(W, kinetic, terms, chunks[c][0], shared.get("out"))
        return ()

    def stage_M(c, s):
        species, blocks = now(species_index, coupling)
        first_atom = band * block // NPA
        shared["matrix"] = mixing_matrix(species, blocks, first_atom, block // NPA)
        return (shared["matrix"],)

    stages = dict(
        Wd=stage_Wd, We=stage_We, T=stage_T, M=stage_M, Wf=stage_Wf, A=stage_A, B=stage_B, C=stage_C,
        E=stage_E, G=stage_G, K=stage_K, H=stage_H, I=stage_I,
    )
    for name, c in stage_order(len(chunks)):
        clock[0] = stages[name](c, state[c])
    return shared["out"]


def solution(mesh):
    in_specs = (P("band", "ga"), P("band", "ga"), P("ga"), P(), P())
    out_specs = P("band", "ga")
    nband, nga = mesh.shape["band"], mesh.shape["ga"]
    square = nband == 4 and nga >= 4 and nga & (nga - 1) == 0

    def local(*args):
        return local_square(nga, *args) if square else local_any(*args)

    def step(*args):
        f = jax.shard_map(
            local, mesh=mesh, in_specs=in_specs, out_specs=out_specs, check_vma=False
        )
        return f(*args)

    return step
```

```python
import functools

import jax
import jax.numpy as jnp
from jax import lax
from jax.experimental import pallas as pl
from jax.experimental.pallas import tpu as pltpu
from jax.sharding import PartitionSpec as P


NPA = 8


def apply_blocks(correlations, species_index, coupling, atom_start):
    rows = correlations.shape[0]
    count = correlations.shape[1] // NPA
    local_species = lax.dynamic_slice_in_dim(species_index, atom_start, count)
    onehot = (
        local_species[:, None] == jnp.arange(coupling.shape[0], dtype=jnp.int32)[None, :]
    ).astype(jnp.float32)
    blocks = jnp.einsum("as,sij->aij", onehot, coupling, precision=lax.Precision.HIGHEST)
    mixed = jnp.einsum(
        "baj,aij->bai",
        correlations.reshape(rows, count, NPA),
        blocks,
        precision=lax.Precision.HIGHEST,
    )
    return mixed.reshape(rows, count * NPA).astype(jnp.bfloat16)


def local_any(wavefunctions, projectors, kinetic_diag, species_index, coupling):
    proj_local = projectors.shape[0]
    partial_value = jnp.einsum(
        "bg,pg->bp",
        lax.all_gather(wavefunctions, "band", axis=0, tiled=True),
        projectors,
        preferred_element_type=jnp.float32,
    )
    total = lax.psum(partial_value.astype(jnp.bfloat16), "ga").astype(jnp.float32)
    first_atom = lax.axis_index("band") * proj_local // NPA
    mixed = apply_blocks(total, species_index, coupling, first_atom)
    nonlocal_term = lax.psum_scatter(
        jnp.dot(mixed, projectors, preferred_element_type=jnp.float32).astype(jnp.bfloat16),
        "band",
        scatter_dimension=0,
        tiled=True,
    ).astype(jnp.float32)
    return (kinetic_diag[None, :] * wavefunctions.astype(jnp.float32) + nonlocal_term).astype(
        jnp.bfloat16
    )


def swap(parts, bit, flag):
    return [jnp.where(flag, parts[i ^ bit], part) for i, part in enumerate(parts)]


def mixing_matrix(species_index, coupling, first_atom, count):
    species = lax.dynamic_slice_in_dim(species_index, first_atom, count)
    onehot = (
        species[:, None] == jnp.arange(coupling.shape[0], dtype=jnp.int32)[None, :]
    ).astype(jnp.float32)
    blocks = jnp.einsum("as,sij->aji", onehot, coupling, precision=lax.Precision.HIGHEST)
    tall = blocks.reshape(count * NPA, NPA)
    wide = jnp.tile(tall, (1, count))
    size = count * NPA
    row = lax.broadcasted_iota(jnp.int32, (size, size), 0) // NPA
    col = lax.broadcasted_iota(jnp.int32, (size, size), 1) // NPA
    return jnp.where(row == col, wide, 0.0)


def chunk_rows(rows, ga):
    unit = max(32, ga * 4)
    if rows % (4 * unit) or ga % 8:
        return [(0, rows)], [(0, 0, 1)]
    return [(0, rows // 2), (rows // 2, rows // 2)], [(0, 0, 1), (1, 0, 2), (1, 1, 2)]


def stage_order(outputs):
    n, parts = outputs[-1][0] + 1, range(len(outputs))
    order = [("Wd", 0), ("We", 0), ("T", 0), ("Wf", 0), ("Wd", 1), ("We", 1), ("M", 0)]
    order += [("A", 0), ("B", 0), ("Wf", 1)]
    for c in range(n):
        order += [("A", c), ("B", c), ("C", c)]
        order += [("H", k) for k in parts if outputs[k][0] == c - 1]
        order += [("E", c)]
        order += [(stage, k) for k in parts if outputs[k][0] == c for stage in ("G", "K")]
    order += [("I", k) for k in parts if outputs[k][0] < n - 1]
    order += [("H", k) for k in parts if outputs[k][0] == n - 1]
    order += [("I", k) for k in parts if outputs[k][0] == n - 1]
    return [item for item in dict.fromkeys(order) if item[0] in "GKHI" or item[1] < n]


def tile_of(width, parts=4):
    while parts > 1 and width % (128 * parts):
        parts -= 1
    return width // parts


def piece_row(piece, rows, index, band):
    first = index * piece
    return pl.multiple_of(((first // rows) ^ band) * rows + first % rows, piece)


def transpose_kernel(value, out):
    out[...] = value[...].T


def transpose(value):
    block, width = value.shape
    tile = tile_of(width, 12)
    return pl.pallas_call(
        transpose_kernel,
        grid=(width // tile,),
        in_specs=[pl.BlockSpec((block, tile), lambda k: (0, k))],
        out_specs=pl.BlockSpec((tile, block), lambda k: (k, 0)),
        out_shape=jax.ShapeDtypeStruct((width, block), value.dtype),
        cost_estimate=pl.CostEstimate(
            flops=16 * block * width, bytes_accessed=4 * block * width, transcendentals=0
        ),
        name="transpose",
    )(value)


def halves_kernel(value, first, second):
    half = first.shape[0]
    first[...] = value[:half]
    second[...] = value[half:]


def take_halves(value, first, count):
    width = value.shape[1]
    tile = tile_of(width, 2)
    return pl.pallas_call(
        halves_kernel,
        grid=(width // tile,),
        in_specs=[pl.BlockSpec((count, tile), lambda k: (first // count, k))],
        out_specs=[pl.BlockSpec((count // 2, tile), lambda k: (0, k))] * 2,
        out_shape=[jax.ShapeDtypeStruct((count // 2, width), value.dtype)] * 2,
        cost_estimate=pl.CostEstimate(
            flops=count * width, bytes_accessed=4 * count * width, transcendentals=0
        ),
        name="take",
    )(value)


def join_kernel(a, b, c, d, first, second):
    f32 = jnp.float32
    first[...] = (a[...].astype(f32) + b[...].astype(f32)).astype(first.dtype)
    second[...] = (c[...].astype(f32) + d[...].astype(f32)).astype(second.dtype)


def join(a, b, c, d):
    half, width = a.shape
    tile = tile_of(width, 2)
    spec = pl.BlockSpec((half, tile), lambda k: (0, k))
    return pl.pallas_call(
        join_kernel,
        grid=(width // tile,),
        in_specs=[spec] * 4,
        out_specs=[spec] * 2,
        out_shape=[jax.ShapeDtypeStruct(a.shape, a.dtype)] * 2,
        cost_estimate=pl.CostEstimate(
            flops=2 * half * width, bytes_accessed=12 * half * width, transcendentals=0
        ),
        name="join",
    )(a, b, c, d)


def finish_kernel(bands, kinetic, *refs):
    terms, out = refs[:6], refs[-1]
    half = terms[0].shape[0]
    f32 = jnp.float32
    for k in range(2):
        rows = slice(k * half, (k + 1) * half)
        own = sum(term[...].astype(f32) for term in terms[k::2])
        out[rows] = (kinetic[...] * bands[rows].astype(f32) + own).astype(out.dtype)


def finish(bands, kinetic, terms, first, out):
    half, width = terms[0].shape
    count = 2 * half
    tile = tile_of(width, 2)
    rows = pl.BlockSpec((count, tile), lambda k: (first // count, k))
    part = pl.BlockSpec((half, tile), lambda k: (0, k))
    args = [bands, kinetic[None, :], *terms]
    specs = [rows, pl.BlockSpec((1, tile), lambda k: (0, k))] + [part] * 6
    aliases = {}
    if out is not None:
        aliases = {len(args): 0}
        args.append(out)
        specs.append(pl.BlockSpec(memory_space=pl.ANY))
    return pl.pallas_call(
        finish_kernel,
        grid=(width // tile,),
        in_specs=specs,
        out_specs=rows,
        out_shape=jax.ShapeDtypeStruct(bands.shape, bands.dtype),
        input_output_aliases=aliases,
        cost_estimate=pl.CostEstimate(
            flops=8 * count * width, bytes_accessed=10 * count * width, transcendentals=0
        ),
        name="finish",
    )(*args)


def correlate_kernel(nz, where, *refs):
    halves, (proj, kept, sent, acc) = refs[:8], refs[8:]
    step = pl.program_id(0)
    band, core = where[0], where[1]
    bands = jnp.concatenate([half[...] for half in halves], axis=0)
    part = jnp.dot(bands, proj[...], preferred_element_type=jnp.float32)

    @pl.when(step == 0)
    def _():
        acc[...] = part

    @pl.when(step > 0)
    def _():
        acc[...] += part

    @pl.when(step == pl.num_programs(0) - 1)
    def _():
        rows = 2 * halves[0].shape[0]
        piece = kept.shape[1]
        for k in range(nz):
            at = piece_row(piece, rows, 2 * k + core, band)
            kept[k] = acc[pl.ds(at, piece), :].astype(kept.dtype)
            at = piece_row(piece, rows, 2 * k + 1 - core, band)
            sent[k] = acc[pl.ds(at, piece), :].astype(sent.dtype)


def correlate(where, nz, halves, proj):
    half, width = halves[0].shape
    block = proj.shape[1]
    piece = 8 * half // (2 * nz)
    tile = tile_of(width)
    out = jax.ShapeDtypeStruct((nz, piece, block), jnp.bfloat16)
    whole = pl.BlockSpec((nz, piece, block), lambda k, w: (0, 0, 0))
    return pl.pallas_call(
        functools.partial(correlate_kernel, nz),
        grid_spec=pltpu.PrefetchScalarGridSpec(
            num_scalar_prefetch=1,
            grid=(width // tile,),
            in_specs=[pl.BlockSpec((half, tile), lambda k, w: (0, k))] * 8
            + [pl.BlockSpec((tile, block), lambda k, w: (k, 0))],
            out_specs=[whole, whole],
            scratch_shapes=[pltpu.VMEM((8 * half, block), jnp.float32)],
        ),
        out_shape=[out, out],
        cost_estimate=pl.CostEstimate(
            flops=16 * half * width * block,
            bytes_accessed=2 * (8 * half + block) * width,
            transcendentals=0,
        ),
        name="correlate",
    )(where, *halves, proj)


def expand_kernel(nz, part, where, here, there, proj, *refs):
    outs, (pieces, mixed) = refs[:8], refs[8:]
    band, core = where[0], where[1]
    half = outs[0].shape[0]
    sub, count = part
    rows = 2 * half * count
    piece = here.shape[1]
    each = 2 * half // piece
    picked = [(k * count + sub) * each + i for k in range(4) for i in range(each)]

    @pl.when(pl.program_id(0) == 0)
    def _():
        for k in range(nz):
            pieces[piece_row(piece, rows, 2 * k + core, band) // piece] = here[k]
            pieces[piece_row(piece, rows, 2 * k + 1 - core, band) // piece] = there[k]
        mixed[...] = jnp.concatenate([pieces[k] for k in picked], axis=0)

    value = jnp.dot(mixed[...], proj[...], preferred_element_type=jnp.float32)
    for k, out in enumerate(outs):
        out[...] = value[k * half : (k + 1) * half].astype(out.dtype)


def expand(where, nz, part, rows, here, there, proj):
    block, width = proj.shape
    piece = here.shape[1]
    tile = tile_of(width)
    whole = pl.BlockSpec((nz, piece, block), lambda k, w: (0, 0, 0))

    def out(count):
        return jax.ShapeDtypeStruct((count, width), jnp.bfloat16)

    def spec(count):
        return pl.BlockSpec((count, tile), lambda k, w: (0, k))

    counts = [rows // 2] * 8
    return pl.pallas_call(
        functools.partial(expand_kernel, nz, part),
        grid_spec=pltpu.PrefetchScalarGridSpec(
            num_scalar_prefetch=1,
            grid=(width // tile,),
            in_specs=[whole, whole, spec(block)],
            out_specs=[spec(n) for n in counts],
            scratch_shapes=[
                pltpu.VMEM((2 * nz, piece, block), jnp.bfloat16),
                pltpu.VMEM((4 * rows, block), jnp.bfloat16),
            ],
        ),
        out_shape=[out(n) for n in counts],
        cost_estimate=pl.CostEstimate(
            flops=8 * rows * width * block,
            bytes_accessed=2 * (4 * rows + block) * width,
            transcendentals=0,
        ),
        name="expand",
    )(where, here, there, proj)


def local_square(nga, W, Pr, kinetic, species_index, coupling):
    bf, f32 = jnp.bfloat16, jnp.float32
    rows, _ = W.shape
    block = Pr.shape[0]
    nz = nga // 2

    band = lax.axis_index("band")
    ga = lax.axis_index("ga")
    core, z = ga % 2, ga // 2
    where = jnp.stack([band, core])

    def band_swap(value, bit):
        return lax.ppermute(value, "band", [(i, i ^ bit) for i in range(4)])

    def ga_swap(value, bit):
        return lax.ppermute(value, "ga", [(i, i ^ bit) for i in range(nga)])

    chunks, outputs = chunk_rows(rows, nga)
    clock = [()]

    def now(*values):
        out = lax.optimization_barrier((*values, *clock[0]))
        return out[: len(values)]

    state = [dict() for _ in chunks]
    made = [dict() for _ in outputs]
    shared = {}

    def stage_Wd(c, s):
        first, count = chunks[c]
        (bands,) = now(W)
        s["own"] = take_halves(bands, first, count)
        s["x0"] = band_swap(s["own"][0], 1)
        s["y1"] = band_swap(s["own"][1], 2)
        return tuple(s["own"])

    def stage_We(c, s):
        own = now(*s["own"])
        s["x1"] = band_swap(own[1], 1)
        s["y0"] = band_swap(own[0], 2)
        return tuple(own)

    def stage_T(c, s):
        (turned,) = now(Pr)
        shared["turned"] = transpose(turned)
        return (shared["turned"],)

    def stage_Wf(c, s):
        x0, y1 = now(s["x0"], s["y1"])
        s["far0"] = band_swap(x0, 2)
        s["far1"] = band_swap(y1, 1)
        return x0, y1

    def stage_A(c, s):
        x1, y0, far0, far1 = now(s["x1"], s["y0"], s["far0"], s["far1"])
        halves = [*s["own"], s["x0"], x1, y0, s["y1"], far0, far1]
        s["kept"], sent = correlate(where, nz, halves, shared["turned"])
        s["core"] = ga_swap(sent, 1)
        return s["kept"], sent

    def stage_B(c, s):
        (other,) = now(s["core"])
        half = (s["kept"].astype(f32) + other.astype(f32)).astype(bf)
        outs = [
            lax.dynamic_index_in_dim(half, z ^ m, 0, keepdims=False) for m in range(1, nz)
        ]
        s["mine"] = lax.dynamic_index_in_dim(half, z, 0, keepdims=False)
        s["z"] = [ga_swap(out, 2 * m) for m, out in enumerate(outs, 1)]
        return tuple(outs)

    def stage_C(c, s):
        parts = now(*s["z"])
        total = s["mine"].astype(f32)
        for part in parts:
            total = total + part.astype(f32)
        mixed = jnp.dot(total, shared["matrix"], precision=lax.Precision.HIGHEST).astype(bf)
        s["mixed"] = [mixed] + [ga_swap(mixed, 2 * m) for m in range(1, nz)]
        return (mixed,)

    def stage_E(c, s):
        parts = list(now(*s["mixed"]))
        bit = 1
        while bit < nz:
            parts = swap(parts, bit, (z & bit) != 0)
            bit *= 2
        s["here"] = jnp.stack(parts)
        s["there"] = ga_swap(s["here"], 1)
        return (s["here"],)

    def stage_G(c, s):
        chunk, sub, count = outputs[c]
        here, there = now(state[chunk]["here"], state[chunk]["there"])
        rows = chunks[chunk][1] // count
        s["first"] = chunks[chunk][0] + sub * rows
        s["o"] = expand(where, nz, (sub, count), rows, here, there, Pr)
        s["first_y"] = band_swap(s["o"][6], 2)
        s["first_x"] = band_swap(s["o"][7], 1)
        return s["o"][6], s["o"][7]

    def stage_K(c, s):
        to_y, to_x = now(s["o"][4], s["o"][3])
        s["near0"] = band_swap(to_y, 2)
        s["near1"] = band_swap(to_x, 1)
        return to_y, to_x

    def stage_H(c, s):
        first_x, first_y = now(s["first_x"], s["first_y"])
        to_x, to_y = join(s["o"][2], first_y, s["o"][5], first_x)
        s["second0"] = band_swap(to_x, 1)
        s["second1"] = band_swap(to_y, 2)
        return to_x, to_y

    def stage_I(c, s):
        parts = now(s["near0"], s["near1"], s["second0"], s["second1"])
        terms = [s["o"][0], s["o"][1], *parts]
        shared["out"] = finish(W, kinetic, terms, s["first"], shared.get("out"))
        return ()

    def stage_M(c, s):
        species, blocks = now(species_index, coupling)
        first_atom = band * block // NPA
        shared["matrix"] = mixing_matrix(species, blocks, first_atom, block // NPA)
        return (shared["matrix"],)

    stages = dict(
        Wd=stage_Wd, We=stage_We, T=stage_T, M=stage_M, Wf=stage_Wf, A=stage_A, B=stage_B, C=stage_C,
        E=stage_E, G=stage_G, K=stage_K, H=stage_H, I=stage_I,
    )
    for name, c in stage_order(outputs):
        clock[0] = stages[name](c, (made if name in "GKHI" else state)[c])
    return shared["out"]


def solution(mesh):
    in_specs = (P("band", "ga"), P("band", "ga"), P("ga"), P(), P())
    out_specs = P("band", "ga")
    nband, nga = mesh.shape["band"], mesh.shape["ga"]
    square = nband == 4 and nga >= 4 and nga & (nga - 1) == 0

    def local(*args):
        return local_square(nga, *args) if square else local_any(*args)

    def step(*args):
        f = jax.shard_map(
            local, mesh=mesh, in_specs=in_specs, out_specs=out_specs, check_vma=False
        )
        return f(*args)

    return step
```
